512 devices in a mesh: seq: 128 (over z, x, core), head: 4 (over y).
Axes of the slice: x: 4, y: 4, z: 16, core: 2. Of those that a mesh axis runs over, the one named last changes fastest.
Arguments:
- x_in: bfloat16 [32768, 5120], P('seq', 'head'), may hold values from -6 to 6
- bc_in: bfloat16 [32768, 256], P('seq'), may hold values from -6 to 6
- z_in: bfloat16 [32768, 5120], P('seq', 'head'), may hold values from -6 to 6
- dt_raw: float32 [80, 32768], P('head', 'seq'), may hold values from -3 to 3
- dt_bias: float32 [80], P('head'), may hold values from -2.8 to -1.7
- a_log: float32 [80], P('head'), as said below
- conv_x: float32 [4, 5120], P(None, 'head'), may hold values from -3 to 3
- conv_bc: float32 [4, 256], replicated, may hold values from -3 to 3
- conv_x_bias: float32 [5120], P('head'), may hold values from -3 to 3
- conv_bc_bias: float32 [256], replicated, may hold values from -3 to 3
- norm_weight: float32 [5120], P('head'), may hold values from 0.1 to 1.9
Outputs:
- y_out: bfloat16 [32768, 5120], P('seq', 'head')
The draws below stay inside these ranges and needn't reach their ends.
Inputs may be any that keep to these rules, and one draw needn't show every extreme that they name: a_log is at least log(2 / 32768) and at most 0.
All inputs are finite; a program needn't handle non-finite values.
Results may differ from the reference program's by a relative error of at most 0.012.
Values may be sent and summed in bfloat16 or wider, within the bound.
A program may use at most 128 MiB of HBM per device.

```python
import jax
import jax.numpy as jnp
from jax import lax

HEADS = 80
HEADDIM = 64
STATE = 128
CONV = 4
SPAN = 256
SEQLEN = 32768
INNER = 5120


def draw_a_log(key, part):
    key_slow = jax.random.fold_in(key, 11)
    key_fast = jax.random.fold_in(key, 12)
    key_pick = jax.random.fold_in(key, 13)
    slow_rates = jax.random.uniform(key_slow, (HEADS,), jnp.float32, jnp.log(2.0 / SEQLEN), jnp.log(8.0 / SEQLEN))
    fast_rates = jax.random.uniform(key_fast, (HEADS,), jnp.float32, jnp.log(0.3), 0.0)
    chosen = jax.random.randint(key_pick, (HEADS,), 0, 10)
    picked = chosen < 5
    return jnp.where(picked, fast_rates, slow_rates)


def level_of(own_key, shape, split, smallest, top_value):
    loudness, own = 1.0, jax.random.fold_in(own_key, 6)
    for axis_at, parts in split:
        heights = jnp.exp(jax.random.uniform(jax.random.fold_in(own, axis_at), (parts,), jnp.float32, smallest / len(split), top_value / len(split)))
        loudness = loudness * jnp.repeat(heights, shape[axis_at] // parts).reshape([-1 if axis == axis_at else 1 for axis in range(len(shape))])
    return loudness


def scatter_about(stream_key, dims, width, bound, cuts=(), dtype=jnp.bfloat16):
    factor_of = level_of(stream_key, dims, cuts, -0.22, 0.18) if cuts else 1.0
    array = jax.random.normal(stream_key, dims, jnp.float32) * width * factor_of
    return jnp.minimum(jnp.maximum(array, -bound), bound).astype(dtype)


def setup_inputs(seed: int = 0) -> dict:
    splits = jax.random.split(jax.random.key(seed), 12)
    x_in = scatter_about(splits[0], (SEQLEN, INNER), 1.0, 6.0, ((0, 128), (1, 4)))
    bc_in = scatter_about(splits[1], (SEQLEN, 2 * STATE), 1.0, 6.0, ((0, 128),))
    z_in = scatter_about(splits[2], (SEQLEN, INNER), 1.0, 6.0, ((0, 128), (1, 4)))
    dt_raw = scatter_about(splits[3], (HEADS, SEQLEN), 0.5, 3.0, ((0, 4), (1, 128)), jnp.float32)
    dt_bias = jnp.clip(-2.8 + 1.0999999 * jax.random.uniform(splits[4], (HEADS,), jnp.float32) ** level_of(splits[4], (HEADS,), ((0, 4),), -0.2, 0.2), -2.8, -1.7)
    a_log = draw_a_log(jax.random.fold_in(splits[11], 71), 0)
    conv_x = scatter_about(splits[6], (CONV, INNER), CONV ** -0.5, 3.0, ((1, 4),), jnp.float32)
    conv_bc = scatter_about(splits[7], (CONV, 2 * STATE), CONV ** -0.5, 3.0, (), jnp.float32)
    conv_x_bias = scatter_about(splits[8], (INNER,), 0.5, 3.0, ((0, 4),), jnp.float32)
    conv_bc_bias = scatter_about(splits[9], (2 * STATE,), 0.5, 3.0, (), jnp.float32)
    norm_weight = jnp.clip(1.0 + 0.18 * jax.random.normal(splits[10], (INNER,), jnp.float32), 0.1, 1.9)
    return {"x_in": x_in, "bc_in": bc_in, "z_in": z_in, "dt_raw": dt_raw, "dt_bias": dt_bias, "a_log": a_log, "conv_x": conv_x, "conv_bc": conv_bc, "conv_x_bias": conv_x_bias, "conv_bc_bias": conv_bc_bias, "norm_weight": norm_weight}


def causal_conv(source, rim_rows, taps, conv_bias):
    tok_rows = source.shape[0]
    padded = jnp.concatenate([rim_rows, source], axis=0).astype(jnp.float32)
    running = conv_bias[None, :] + taps[0][None, :] * padded[0:tok_rows]
    for offset in range(1, taps.shape[0]):
        running = running + taps[offset][None, :] * padded[offset:offset + tok_rows]
    return jax.nn.silu(running).astype(jnp.bfloat16)

def span_terms(x_blk, b_blk, c_blk, step_blk, cumulative):
    length = c_blk.shape[0]
    scores = jnp.dot(c_blk, b_blk.T, preferred_element_type=jnp.float32)
    causal = jnp.arange(length)[:, None] >= jnp.arange(length)[None, :]
    log_gap = jnp.where(causal[None], cumulative[:, :, None] - cumulative[:, None, :], 0.0)
    mixing = jnp.where(causal[None], scores[None] * jnp.exp(log_gap) * step_blk[:, None, :], 0.0).astype(jnp.bfloat16)
    y_inner = jnp.einsum('htj,jhp->thp', mixing.astype(jnp.float32), x_blk.astype(jnp.float32))
    weight_in = jnp.exp(cumulative[:, -1:] - cumulative) * step_blk
    x_weighted = (x_blk.astype(jnp.float32) * weight_in.T[:, :, None]).astype(jnp.bfloat16)
    state_part = jnp.einsum('jhp,jn->hpn', x_weighted.astype(jnp.float32), b_blk.astype(jnp.float32))
    return (y_inner, state_part)

def reference(x_in, bc_in, z_in, dt_raw, dt_bias, a_log, conv_x, conv_bc, conv_x_bias, conv_bc_bias, norm_weight):
    x_conv = causal_conv(x_in, jnp.zeros((CONV - 1, x_in.shape[1]), jnp.bfloat16), conv_x, conv_x_bias)
    bc_conv = causal_conv(bc_in, jnp.zeros((CONV - 1, bc_in.shape[1]), jnp.bfloat16), conv_bc, conv_bc_bias)
    step_size = jax.nn.softplus(dt_raw + dt_bias[:, None])
    log_decay = step_size * (-jnp.exp(a_log))[:, None]
    span_count = SEQLEN // SPAN
    x_blocks = x_conv.reshape(span_count, SPAN, HEADS, HEADDIM)
    b_blocks = bc_conv[:, :STATE].reshape(span_count, SPAN, STATE)
    c_blocks = bc_conv[:, STATE:].reshape(span_count, SPAN, STATE)
    step_blocks = step_size.reshape(HEADS, span_count, SPAN).transpose(1, 0, 2)
    decay_blocks = log_decay.reshape(HEADS, span_count, SPAN).transpose(1, 0, 2)

    def advance(carried, inputs):
        x_blk, b_blk, c_blk, step_blk, decay_blk = inputs
        cumulative = jnp.cumsum(decay_blk, axis=1)
        y_inner, state_part = span_terms(x_blk, b_blk, c_blk, step_blk, cumulative)
        y_outer = jnp.einsum('tn,hpn->thp', c_blk.astype(jnp.float32), carried, precision=lax.Precision.HIGHEST)
        y_outer = y_outer * jnp.exp(cumulative).T[:, :, None]
        updated = jnp.exp(cumulative[:, -1])[:, None, None] * carried + state_part
        return (updated, y_inner + y_outer)
    final_state, y_blocks = lax.scan(advance, jnp.zeros((HEADS, HEADDIM, STATE), jnp.float32), (x_blocks, b_blocks, c_blocks, step_blocks, decay_blocks))
    y_full = y_blocks.reshape(SEQLEN, HEADS * HEADDIM)
    gated_rows = y_full * jax.nn.silu(z_in.astype(jnp.float32))
    squares = lax.optimization_barrier(jnp.sum(gated_rows * gated_rows, axis=1))
    inv_rms = lax.rsqrt(squares / (HEADS * HEADDIM) + 1e-05)
    return (gated_rows * inv_rms[:, None] * norm_weight[None, :]).astype(jnp.bfloat16)
```

```python
import functools

import jax
import jax.numpy as jnp
from jax import lax
from jax.experimental import pallas as pl
from jax.experimental.pallas import tpu as pltpu
from jax.sharding import Mesh
from jax.sharding import PartitionSpec as P

HEADDIM = 64
STATE = 128
CONV = 4
RIM = 16
GROUP = 3
EARLY_TILES = 6
AXES = ("seq_0", "seq_1", "seq_2", "head")
SEQ = AXES[:3]
F32 = jnp.float32
BF16 = jnp.bfloat16


def dot(a, b, contract=((1,), (0,)), precision=None):
    return lax.dot_general(
        a, b, (contract, ((), ())), preferred_element_type=F32, precision=precision
    )


def silu(value):
    return value / (1.0 + jnp.exp(-value))


def split_two(value):
    high = value.astype(BF16)
    low = (value - high.astype(F32)).astype(BF16)
    return jnp.concatenate([high, low], axis=1)


def split_three(value):
    high = value.astype(BF16)
    rest = value - high.astype(F32)
    mid = rest.astype(BF16)
    low = (rest - mid.astype(F32)).astype(BF16)
    return jnp.concatenate([high, mid, low], axis=1)


def layer_kernel(sizes, *refs):
    nz, nx, nc, ny, tok, heads, inner = sizes
    (
        x_hbm, bc_hbm, z_hbm, dt_hbm, bias_hbm, alog_hbm, cx_hbm, cbc_hbm, cxb_hbm, cbcb_hbm,
        nw_hbm, out_ref,
        x_v, bc_v, z_v, dt_v, bias_v, alog_v, cx_v, cbc_v, cxb_v, cbcb_v, nw_v,
        xrim, bcrim, xf, bcf, xc, xw, wrim, bmat_t, cmat, scores, dtp, smallp,
        cum_row, step_row, win2, ecum2, cum3, yg, eg, gz,
        stbuf, p1buf, dself, dbuf, pbuf, cumd, tbuf, dplane, abuf, adec,
        pst, fpre, qst, fall, ebuf, ech, obuf, ent, nself, nbuf,
        in_sem, rim_s, rim_r, p1s, p1r, d1s, d1r, as_, ar, ds_, dr, es, er, p3s, p3r, ns_, nr_,
    ) = refs
    tiles = inner // 128
    half = inner // 2
    plane = nx * nc
    rows = STATE // plane
    z = lax.axis_index("seq_0")
    x = lax.axis_index("seq_1")
    c = lax.axis_index("seq_2")
    y = lax.axis_index("head")
    k = x * nc + c
    zl = lax.rem(z, GROUP)

    def remote(source, target, send, recv, device):
        return pltpu.make_async_remote_copy(
            src_ref=source, dst_ref=target, send_sem=send, recv_sem=recv,
            device_id=device, device_id_type=pl.DeviceIdType.MESH,
        )

    def peer_in_plane(other):
        return (z, lax.div(other, nc), lax.rem(other, nc), y)

    def peer_along(other):
        return (other, x, c, y)

    def peer_head(other):
        return (z, x, c, other)

    last_in_plane = k == plane - 1
    first_in_plane = k == 0
    following = lax.rem(k + 1, plane)
    next_z = jnp.where(last_in_plane, z + 1, z)
    next_dev = (next_z, lax.div(following, nc), lax.rem(following, nc), y)
    gives_rim = jnp.logical_or(z < nz - 1, k < plane - 1)
    takes_rim = jnp.logical_or(z > 0, k > 0)
    reach = jnp.minimum(jnp.where(zl == 0, 2, jnp.where(zl == 1, 1, GROUP)), nz - 1 - z)

    with jax.named_scope("a_start"):
        pairs = (
            (x_hbm, x_v), (bc_hbm, bc_v), (dt_hbm, dt_v), (bias_hbm, bias_v), (alog_hbm, alog_v),
            (cx_hbm, cx_v), (cbc_hbm, cbc_v), (cxb_hbm, cxb_v), (cbcb_hbm, cbcb_v), (z_hbm, z_v),
            (nw_hbm, nw_v),
        )
        loads = [
            pltpu.make_async_copy(a, b if len(a.shape) > 1 else b.at[0], in_sem.at[i])
            for i, (a, b) in enumerate(pairs)
        ]
        for i in (2, 3, 4, 0, 5, 7, 1, 6, 8, 9, 10):
            loads[i].start()

        barrier = pltpu.get_barrier_semaphore()

        def greet(device):
            pl.semaphore_signal(
                barrier, inc=1, device_id=device, device_id_type=pl.DeviceIdType.MESH
            )

        for d in range(1, GROUP + 1):

            @pl.when(jnp.logical_and(zl >= d - 1, z >= d))
            def _():
                greet(peer_along(z - d))

        @pl.when(jnp.logical_and(first_in_plane, z > 0))
        def _():
            greet((z - 1, nx - 1, nc - 1, y))

        for d in range(1, plane):
            greet(peer_in_plane(lax.rem(k + d, plane)))
        for d in range(1, ny):
            greet(peer_head(lax.rem(y + d, ny)))
        dtp[...] = jnp.zeros_like(dtp)
        smallp[...] = jnp.zeros_like(smallp)
        xf[0:8, :] = jnp.zeros((8, inner), F32)
        for i in (2, 3, 4):
            loads[i].wait()

    with jax.named_scope("b_dt"):
        dtp[0:heads, :] = dt_v[...]
        smallp[0:1, 0:heads] = bias_v[...]
        smallp[8:9, 0:heads] = alog_v[...]
        raw = jnp.transpose(dtp[...]) + smallp[0:1, :]
        step_t = jnp.maximum(raw, 0.0) + jnp.log1p(jnp.exp(-jnp.abs(raw)))
        decay_t = step_t * (-jnp.exp(smallp[8:9, :]))
        tok_i = lax.broadcasted_iota(jnp.int32, (tok, tok), 0)
        tok_j = lax.broadcasted_iota(jnp.int32, (tok, tok), 1)
        causal = tok_i >= tok_j
        lower = jnp.where(causal, 1.0, 0.0).astype(F32)
        cum_t = dot(lower, decay_t, precision=lax.Precision.HIGHEST)
        cum_row[...] = jnp.transpose(cum_t)
        step_row[...] = jnp.transpose(step_t)
        total = cum_t[tok - 1 : tok, :]
        win2[...] = split_two(jnp.exp(total - cum_t) * step_t)
        ecum2[...] = split_two(jnp.exp(cum_t))
        cum3[...] = split_three(cum_t)
        dself[...] = jnp.broadcast_to(total, dself.shape)

    def spread(tile, depth):
        row = lax.broadcasted_iota(jnp.int32, (128 * depth, 128), 0)
        col = lax.broadcasted_iota(jnp.int32, (128 * depth, 128), 1)
        head = tile * 2 + lax.div(col, HEADDIM)
        return jnp.where(lax.rem(row, 128) == head, 1.0, 0.0).astype(BF16)

    def conv(source, count, taps, bias, lanes):
        running = bias[:, lanes] + taps[0:1, lanes] * source[5 : 5 + count, lanes]
        for offset in range(1, CONV):
            start = 5 + offset
            running = running + taps[offset : offset + 1, lanes] * source[start : start + count, lanes]
        return silu(running).astype(BF16)

    with jax.named_scope("c_conv"):
        for i in (0, 5, 7):
            loads[i].wait()

        def conv_tile(tile, carry):
            lanes = pl.ds(pl.multiple_of(tile * 128, 128), 128)
            xf[8 : 8 + tok, lanes] = x_v[:, lanes].astype(F32)
            x_tile = conv(xf, tok, cx_v, cxb_v, lanes)
            xc[:, lanes] = x_tile
            weight = dot(win2[...], spread(tile, 2))
            wrim[:, lanes] = weight[0:RIM, :]
            xw[:, lanes] = (x_tile.astype(F32) * weight).astype(BF16)
            return carry

        lax.fori_loop(0, tiles, conv_tile, 0, unroll=2)
        for i in (1, 6, 8):
            loads[i].wait()
        bcf[8 : 8 + tok, :] = bc_v[...].astype(F32)

    with jax.named_scope("d_barrier"):
        extra = jnp.where(jnp.logical_and(last_in_plane, z < nz - 1), 1, 0)
        pl.semaphore_wait(barrier, (plane - 1) + (ny - 1) + reach + extra)

    with jax.named_scope("e_rim"):
        rim_copies = [
            remote(x_v.at[pl.ds(tok - RIM, RIM), :], xrim, rim_s.at[0], rim_r.at[0], next_dev),
            remote(bc_v.at[pl.ds(tok - RIM, RIM), :], bcrim, rim_s.at[1], rim_r.at[1], next_dev),
        ]

        @pl.when(gives_rim)
        def _():
            for copy in rim_copies:
                copy.start()

        loads[9].wait()
        loads[10].wait()

        def gate_tile(tile, carry):
            lanes = pl.ds(pl.multiple_of(tile * 128, 128), 128)
            gate = silu(z_v[:, lanes].astype(F32))
            gz[:, lanes] = gate
            eg[:, lanes] = gate * dot(ecum2[...], spread(tile, 2))
            return carry

        lax.fori_loop(0, tiles, gate_tile, 0, unroll=2)

        @pl.when(takes_rim)
        def _():
            for copy in rim_copies:
                copy.wait_recv()
            xf[0:8, :] = xrim[...].astype(F32)[RIM - 8 :, :]
            bcf[0:8, :] = bcrim[...].astype(F32)[RIM - 8 :, :]

        @pl.when(jnp.logical_not(takes_rim))
        def _():
            xf[0:8, :] = jnp.zeros((8, inner), F32)
            bcf[0:8, :] = jnp.zeros((8, 2 * STATE), F32)

    with jax.named_scope("f_state"):
        b_conv = conv(bcf, tok, cbc_v, cbcb_v, slice(0, STATE))
        c_conv = conv(bcf, tok, cbc_v, cbcb_v, slice(STATE, 2 * STATE))
        cmat[...] = c_conv
        bmat_t[...] = jnp.transpose(b_conv.astype(F32)).astype(BF16)
        first = conv(xf, RIM, cx_v, cxb_v, slice(0, inner))
        xc[0:RIM, :] = first
        xw[0:RIM, :] = (first.astype(F32) * wrim[...]).astype(BF16)
        plane_copies = []
        for part in range(2):
            lanes = slice(part * half, part * half + half)
            state = dot(bmat_t[...], xw[:, lanes])
            stbuf[part] = state.reshape(plane, rows, half).astype(BF16)
            for d in range(1, plane):
                other = lax.rem(k + d, plane)
                device = peer_in_plane(other)
                copies = [
                    remote(
                        stbuf.at[part, other], p1buf.at[part, k],
                        p1s.at[part, d - 1], p1r.at[part, d - 1], device,
                    )
                ]
                if part == 0:
                    copies.append(
                        remote(dself, dbuf.at[k], d1s.at[d - 1], d1r.at[d - 1], device)
                    )
                for copy in copies:
                    copy.start()
                plane_copies += copies
            p1buf[part, pl.ds(k, 1)] = stbuf[part, pl.ds(k, 1)]
        dbuf[pl.ds(k, 1)] = dself[...][None]

    def inner_tile(tile, carry):
        lanes = pl.ds(pl.multiple_of(tile * 128, 128), 128)
        x_tile = xc[:, lanes]
        parts = []
        for side in range(2):
            head = tile * 2 + side
            row = lax.broadcasted_iota(jnp.int32, (384, tok), 0)
            pick = jnp.where(lax.rem(row, 128) == head, 1.0, 0.0).astype(BF16)
            column = dot(cum3[...], pick)
            gap = jnp.minimum(column - cum_row[pl.ds(head, 1), :], 0.0)
            mixing = (scores[...] * jnp.exp(gap) * step_row[pl.ds(head, 1), :]).astype(BF16)
            parts.append(dot(mixing, x_tile))
        lane = lax.broadcasted_iota(jnp.int32, (tok, 128), 1)
        yg[:, lanes] = jnp.where(lane < HEADDIM, parts[0], parts[1]) * gz[:, lanes]
        return carry

    with jax.named_scope("g_inner"):
        scores[...] = jnp.where(causal, dot(c_conv, b_conv, ((1,), (1,))), 0.0)
        split = EARLY_TILES
        lax.fori_loop(0, split, inner_tile, 0)

    with jax.named_scope("h_plane_wait"):
        for copy in plane_copies:
            copy.wait()

    with jax.named_scope("i_plane_scan"):
        spread_row = lax.broadcasted_iota(jnp.int32, (128, inner), 0)
        spread_col = lax.broadcasted_iota(jnp.int32, (128, inner), 1)
        spread_all = jnp.where(spread_row == lax.div(spread_col, HEADDIM), 1.0, 0.0).astype(F32)
        each = jnp.concatenate([dbuf[i, 0:1, :] for i in range(plane)], axis=0)
        before = [jnp.zeros((1, 128), F32)]
        for i in range(1, plane):
            before.append(before[-1] + each[i - 1 : i, :])
        whole = before[-1] + each[plane - 1 : plane, :]
        before = jnp.concatenate(before, axis=0)
        stacked = jnp.concatenate([each, before], axis=0)
        wide = dot(stacked, spread_all, precision=lax.Precision.HIGHEST)
        factor = jnp.exp(wide[0:plane, :])
        cumd[...] = jnp.exp(wide[plane : 2 * plane, :])
        dplane[...] = jnp.broadcast_to(whole, (8, 128))
        for part in range(2):
            lanes = slice(part * half, part * half + half)
            running = jnp.zeros((rows, half), F32)
            for i in range(plane):
                pbuf[i, :, lanes] = running
                running = factor[i : i + 1, lanes] * running + p1buf[part, i].astype(F32)
            tbuf[:, lanes] = running.astype(BF16)
            qst[:, lanes] = running

    def group_copies(slot, d):
        device = peer_along(z + d)
        return (
            remote(tbuf, abuf.at[slot], as_.at[d - 1], ar.at[slot], device),
            remote(dplane, adec.at[slot], ds_.at[d - 1], dr.at[slot], device),
        )

    group_sends = ((0, 2), (0, 1), (1, 1))

    def sends_group(slot, d):
        return jnp.logical_and(zl == slot, z + d < nz)

    with jax.named_scope("j_group_send"):
        for slot, d in group_sends:

            @pl.when(sends_group(slot, d))
            def _():
                for copy in group_copies(slot, d):
                    copy.start()

    with jax.named_scope("k_inner"):
        lax.fori_loop(split, tiles, inner_tile, 0)

    with jax.named_scope("l_group_wait"):

        @pl.when(zl == 0)
        def _():
            pst[...] = jnp.zeros_like(pst)
            fpre[...] = jnp.ones_like(fpre)

        def widened(row):
            return jnp.exp(dot(row, spread_all, precision=lax.Precision.HIGHEST))

        @pl.when(zl == 1)
        def _():
            for copy in group_copies(0, 1):
                copy.wait_recv()
            pst[...] = abuf[0].astype(F32)
            fpre[...] = widened(adec[0])

        @pl.when(zl == 2)
        def _():
            for slot in range(2):
                for copy in group_copies(slot, 1):
                    copy.wait_recv()
            mid = widened(adec[1])[0:1, :]
            own = widened(dplane[...])[0:1, :]
            prefix = mid * abuf[0].astype(F32) + abuf[1].astype(F32)
            pst[...] = prefix
            fpre[...] = widened(adec[0] + adec[1])
            qst[...] = own * prefix + qst[...]
            fall[...] = widened(adec[0] + adec[1] + dplane[...])

    def chain_copy(d):
        return remote(ebuf, ech, es.at[d - 1], er.at[0], peer_along(z + d))

    def sends_chain(d):
        return jnp.logical_and(zl == GROUP - 1, z + d < nz)

    with jax.named_scope("m_chain"):

        @pl.when(z < GROUP)
        def _():
            ech[...] = jnp.zeros_like(ech)

        @pl.when(z >= GROUP)
        def _():
            chain_copy(1).wait_recv()

        @pl.when(sends_chain(1))
        def _():
            ebuf[...] = (fall[0:1, :] * ech[...].astype(F32) + qst[...]).astype(BF16)

        for d in range(GROUP, 0, -1):

            @pl.when(sends_chain(d))
            def _():
                chain_copy(d).start()

    with jax.named_scope("n_back_send"):
        entering = fpre[0:1, :] * ech[...].astype(F32) + pst[...]
        own_rows = pl.ds(pl.multiple_of(k * rows, rows), rows)
        for i in range(plane):
            obuf[i] = (cumd[i : i + 1, :] * entering + pbuf[i]).astype(BF16)
        back = []
        for d in range(1, plane):
            other = lax.rem(k + d, plane)
            back.append(
                remote(
                    obuf.at[other], ent.at[own_rows, :], p3s.at[d - 1], p3r.at[d - 1],
                    peer_in_plane(other),
                )
            )
        for copy in back:
            copy.start()
        ent[own_rows, :] = obuf[pl.ds(k, 1)].reshape(rows, inner)

    with jax.named_scope("o_back_wait"):

        @pl.when(gives_rim)
        def _():
            for copy in rim_copies:
                copy.wait_send()

        for slot, d in group_sends:

            @pl.when(sends_group(slot, d))
            def _():
                for copy in group_copies(slot, d):
                    copy.wait_send()

        for copy in back:
            copy.wait()

    with jax.named_scope("p_outer"):
        squares = jnp.zeros((tok, 128), F32)
        for tile in range(tiles):
            lanes = slice(tile * 128, tile * 128 + 128)
            gated = yg[:, lanes] + eg[:, lanes] * dot(cmat[...], ent[:, lanes])
            yg[:, lanes] = gated
            squares = squares + gated * gated

    with jax.named_scope("q_norm"):
        nself[...] = dot(
            jnp.ones((8, 128), F32), squares, ((1,), (1,)), precision=lax.Precision.HIGHEST
        )
        shared = [
            remote(
                nself, nbuf.at[d - 1], ns_.at[d - 1], nr_.at[d - 1], peer_head(lax.rem(y + d, ny))
            )
            for d in range(1, ny)
        ]
        for copy in shared:
            copy.start()
        for d in range(GROUP, 0, -1):

            @pl.when(sends_chain(d))
            def _():
                chain_copy(d).wait_send()

        for copy in shared:
            copy.wait()
        summed = nself[...]
        for d in range(1, ny):
            summed = summed + nbuf[d - 1]
        inv = lax.rsqrt(summed / (ny * inner) + 1e-05)
        inv = jnp.transpose(jnp.concatenate([inv] * 16, axis=0))

    with jax.named_scope("r_out"):
        for tile in range(tiles):
            lanes = slice(tile * 128, tile * 128 + 128)
            out_ref[:, lanes] = (yg[:, lanes] * inv * nw_v[:, lanes]).astype(BF16)


def local(
    shape,
    x_in,
    bc_in,
    z_in,
    dt_raw,
    dt_bias,
    a_log,
    conv_x,
    conv_bc,
    conv_x_bias,
    conv_bc_bias,
    norm_weight,
):
    nz, nx, nc, ny = shape
    tok, inner = x_in.shape
    heads = dt_raw.shape[0]
    plane = nx * nc
    rows = STATE // plane
    half = inner // 2
    sizes = (nz, nx, nc, ny, tok, heads, inner)
    operands = (
        x_in, bc_in, z_in, dt_raw, dt_bias, a_log, conv_x, conv_bc, conv_x_bias, conv_bc_bias,
        norm_weight,
    )
    v = pltpu.VMEM
    dma = pltpu.SemaphoreType.DMA
    scratch = [v(o.shape if o.ndim > 1 else (1, *o.shape), o.dtype) for o in operands]
    others = max(ny - 1, 1)
    scratch += [
        v((RIM, inner), BF16), v((RIM, 2 * STATE), BF16),
        v((tok + 8, inner), F32), v((tok + 8, 2 * STATE), F32),
        v((tok, inner), BF16), v((tok, inner), BF16), v((RIM, inner), F32),
        v((STATE, tok), BF16), v((tok, STATE), BF16), v((tok, tok), F32),
        v((128, tok), F32), v((16, 128), F32),
        v((128, tok), F32), v((128, tok), F32), v((tok, 256), BF16), v((tok, 256), BF16),
        v((tok, 384), BF16), v((tok, inner), F32), v((tok, inner), F32), v((tok, inner), F32),
        v((2, plane, rows, half), BF16), v((2, plane, rows, half), BF16), v((8, 128), F32),
        v((plane, 8, 128), F32), v((plane, rows, inner), F32), v((plane, inner), F32),
        v((rows, inner), BF16), v((8, 128), F32), v((2, rows, inner), BF16), v((2, 8, 128), F32),
        v((rows, inner), F32), v((8, inner), F32), v((rows, inner), F32), v((8, inner), F32),
        v((rows, inner), BF16), v((rows, inner), BF16),
        v((plane, rows, inner), BF16), v((STATE, inner), BF16),
        v((8, tok), F32), v((others, 8, tok), F32),
        dma((11,)), dma((2,)), dma((2,)),
        dma((2, plane - 1)), dma((2, plane - 1)), dma((plane - 1,)), dma((plane - 1,)),
        dma((2,)), dma((2,)), dma((2,)), dma((2,)),
        dma((GROUP,)), dma((1,)),
        dma((plane - 1,)), dma((plane - 1,)), dma((others,)), dma((others,)),
    ]
    return pl.pallas_call(
        functools.partial(layer_kernel, sizes),
        out_shape=pltpu.VMEM((tok, inner), BF16),
        in_specs=[pl.BlockSpec(memory_space=pltpu.HBM)] * 11,
        out_specs=pl.BlockSpec(memory_space=pltpu.VMEM),
        scratch_shapes=scratch,
        compiler_params=pltpu.CompilerParams(
            collective_id=0, has_side_effects=True, vmem_limit_bytes=66000000
        ),
        name="layer",
    )(*operands)


def build(mesh, shape):
    torus = Mesh(mesh.devices.reshape(shape), AXES)
    return jax.shard_map(
        functools.partial(local, shape),
        mesh=torus,
        in_specs=(
            P(SEQ, "head"),
            P(SEQ, None),
            P(SEQ, "head"),
            P("head", SEQ),
            P("head"),
            P("head"),
            P(None, "head"),
            P(),
            P("head"),
            P(),
            P("head"),
        ),
        out_specs=P(SEQ, "head"),
        check_vma=False,
    )


def solution(mesh):
    return build(mesh, (16, 4, 2, mesh.shape["head"]))
```

```python
import functools

import jax
import jax.numpy as jnp
from jax import lax
from jax.experimental import pallas as pl
from jax.experimental.pallas import tpu as pltpu
from jax.sharding import Mesh
from jax.sharding import PartitionSpec as P

HEADDIM = 64
STATE = 128
CONV = 4
RIM = 16
GROUP = 3
EARLY_TILES = 6
EARLY_CONV = 4
AXES = ("seq_0", "seq_1", "seq_2", "head")
SEQ = AXES[:3]
F32 = jnp.float32
BF16 = jnp.bfloat16


def dot(a, b, contract=((1,), (0,)), precision=None):
    return lax.dot_general(
        a, b, (contract, ((), ())), preferred_element_type=F32, precision=precision
    )


def silu(value):
    half = 0.5 * value
    return half + half * jnp.tanh(half)


def split_two(value):
    high = value.astype(BF16)
    low = (value - high.astype(F32)).astype(BF16)
    return jnp.concatenate([high, low], axis=1)


def split_three(value):
    high = value.astype(BF16)
    rest = value - high.astype(F32)
    mid = rest.astype(BF16)
    low = (rest - mid.astype(F32)).astype(BF16)
    return jnp.concatenate([high, mid, low], axis=1)


def layer_kernel(sizes, *refs):
    nz, nx, nc, ny, tok, heads, inner = sizes
    (
        x_hbm, bc_hbm, z_hbm, dt_hbm, bias_hbm, alog_hbm, cx_hbm, cbc_hbm, cxb_hbm, cbcb_hbm,
        nw_hbm, out_ref,
        x_v, bc_v, z_v, dt_v, bias_v, alog_v, cx_v, cbc_v, cxb_v, cbcb_v, nw_v,
        xrim, bcrim, xf, bcf, xc, xw, wrim, bmat_t, cmat, scores, dtp, smallp,
        cum_row, step_row, win2, ecum2, cum3, yg, eg, gz,
        stbuf, p1buf, dself, dbuf, pbuf, cumd, tbuf, dplane, abuf, adec,
        pst, fpre, qst, fall, ebuf, ech, obuf, ent, nself, nbuf,
        in_sem, rim_s, rim_r, p1s, p1r, d1s, d1r, as_, ar, ds_, dr, es, er, p3s, p3r, ns_, nr_,
        ready,
    ) = refs
    tiles = inner // 128
    half = inner // 2
    plane = nx * nc
    rows = STATE // plane
    z = lax.axis_index("seq_0")
    x = lax.axis_index("seq_1")
    c = lax.axis_index("seq_2")
    y = lax.axis_index("head")
    k = x * nc + c
    groups = nz // GROUP
    last_size = nz - GROUP * (groups - 1)
    group = jnp.minimum(lax.div(z, GROUP), groups - 1)
    zl = z - group * GROUP
    hands_on = jnp.logical_and(zl == GROUP - 1, group < groups - 1)

    def remote(source, target, send, recv, device):
        return pltpu.make_async_remote_copy(
            src_ref=source, dst_ref=target, send_sem=send, recv_sem=recv,
            device_id=device, device_id_type=pl.DeviceIdType.MESH,
        )

    def peer_in_plane(other):
        return (z, lax.div(other, nc), lax.rem(other, nc), y)

    def peer_along(other):
        return (other, x, c, y)

    def peer_head(other):
        return (z, x, c, other)

    last_in_plane = k == plane - 1
    first_in_plane = k == 0
    following = lax.rem(k + 1, plane)
    next_z = jnp.where(last_in_plane, z + 1, z)
    next_dev = (next_z, lax.div(following, nc), lax.rem(following, nc), y)
    gives_rim = jnp.logical_or(z < nz - 1, k < plane - 1)
    takes_rim = jnp.logical_or(z > 0, k > 0)
    size = jnp.where(group == groups - 1, last_size, GROUP)
    next_size = jnp.where(group == groups - 2, last_size, GROUP)
    reach = jnp.where(hands_on, next_size, size - 1 - zl)

    def has_source(d):
        return jnp.logical_and(zl >= d - 1, z >= d)

    with jax.named_scope("a_start"):
        pairs = (
            (x_hbm, x_v), (bc_hbm, bc_v), (dt_hbm, dt_v), (bias_hbm, bias_v), (alog_hbm, alog_v),
            (cx_hbm, cx_v), (cbc_hbm, cbc_v), (cxb_hbm, cxb_v), (cbcb_hbm, cbcb_v), (z_hbm, z_v),
            (nw_hbm, nw_v),
        )
        loads = [
            pltpu.make_async_copy(a, b if len(a.shape) > 1 else b.at[0], in_sem.at[i])
            for i, (a, b) in enumerate(pairs)
        ]
        for i in (2, 3, 4, 0, 5, 7, 1, 6, 8, 9, 10):
            loads[i].start()

        barrier = pltpu.get_barrier_semaphore()

        def greet(device):
            pl.semaphore_signal(
                barrier, inc=1, device_id=device, device_id_type=pl.DeviceIdType.MESH
            )

        for d in range(1, last_size + 1):

            @pl.when(d <= reach)
            def _():
                greet(peer_along(z + d))

        @pl.when(jnp.logical_and(first_in_plane, z > 0))
        def _():
            greet((z - 1, nx - 1, nc - 1, y))

        for d in range(1, plane):
            greet(peer_in_plane(lax.rem(k + d, plane)))
        for d in range(1, ny):
            greet(peer_head(lax.rem(y + d, ny)))
        dtp[...] = jnp.zeros_like(dtp)
        smallp[...] = jnp.zeros_like(smallp)
        xf[0:8, :] = jnp.zeros((8, inner), F32)
        for i in (2, 3, 4):
            loads[i].wait()

    with jax.named_scope("b_dt"):
        dtp[0:heads, :] = dt_v[...]
        smallp[0:1, 0:heads] = bias_v[...]
        smallp[8:9, 0:heads] = alog_v[...]
        raw = jnp.transpose(dtp[...]) + smallp[0:1, :]
        step_t = jnp.maximum(raw, 0.0) + jnp.log1p(jnp.exp(-jnp.abs(raw)))
        decay_t = step_t * (-jnp.exp(smallp[8:9, :]))
        tok_i = lax.broadcasted_iota(jnp.int32, (tok, tok), 0)
        tok_j = lax.broadcasted_iota(jnp.int32, (tok, tok), 1)
        causal = tok_i >= tok_j
        lower = jnp.where(causal, 1.0, 0.0).astype(F32)
        cum_t = dot(lower, decay_t, precision=lax.Precision.HIGHEST)
        cum_row[...] = jnp.transpose(cum_t)
        step_row[...] = jnp.transpose(step_t)
        total = cum_t[tok - 1 : tok, :]
        win2[...] = split_two(jnp.exp(total - cum_t) * step_t)
        ecum2[...] = split_two(jnp.exp(cum_t))
        cum3[...] = split_three(cum_t)
        dself[...] = jnp.broadcast_to(total, dself.shape)

    def spread(tile, depth):
        row = lax.broadcasted_iota(jnp.int32, (128 * depth, 128), 0)
        col = lax.broadcasted_iota(jnp.int32, (128 * depth, 128), 1)
        head = tile * 2 + lax.div(col, HEADDIM)
        return jnp.where(lax.rem(row, 128) == head, 1.0, 0.0).astype(BF16)

    def conv(source, count, taps, bias, lanes):
        running = bias[:, lanes] + taps[0:1, lanes] * source[5 : 5 + count, lanes]
        for offset in range(1, CONV):
            start = 5 + offset
            running = running + taps[offset : offset + 1, lanes] * source[start : start + count, lanes]
        return silu(running).astype(BF16)

    with jax.named_scope("c_conv"):
        for i in (0, 5, 7):
            loads[i].wait()

        def conv_tile(tile, carry):
            lanes = pl.ds(pl.multiple_of(tile * 128, 128), 128)
            xf[8 : 8 + tok, lanes] = x_v[:, lanes].astype(F32)
            x_tile = conv(xf, tok, cx_v, cxb_v, lanes)
            xc[:, lanes] = x_tile
            weight = dot(win2[...], spread(tile, 2))
            wrim[:, lanes] = weight[0:RIM, :]
            xw[:, lanes] = (x_tile.astype(F32) * weight).astype(BF16)
            return carry

        lax.fori_loop(0, EARLY_CONV, conv_tile, 0, unroll=2)
        loads[1].wait()

    with jax.named_scope("d_barrier"):
        extra = jnp.where(jnp.logical_and(last_in_plane, z < nz - 1), 1, 0)
        sources = jnp.minimum(zl + 1, z)
        pl.semaphore_wait(barrier, (plane - 1) + (ny - 1) + sources + extra)

    with jax.named_scope("e_rim"):
        rim_copies = [
            remote(x_v.at[pl.ds(tok - RIM, RIM), :], xrim, rim_s.at[0], rim_r.at[0], next_dev),
            remote(bc_v.at[pl.ds(tok - RIM, RIM), :], bcrim, rim_s.at[1], rim_r.at[1], next_dev),
        ]

        @pl.when(gives_rim)
        def _():
            for copy in rim_copies:
                copy.start()

        for d in range(1, last_size + 1):

            @pl.when(has_source(d))
            def _():
                pl.semaphore_signal(
                    ready.at[d - 1], inc=1, device_id=peer_along(z - d),
                    device_id_type=pl.DeviceIdType.MESH,
                )

        lax.fori_loop(EARLY_CONV, tiles, conv_tile, 0, unroll=2)
        for i in (6, 8):
            loads[i].wait()
        bcf[8 : 8 + tok, :] = bc_v[...].astype(F32)

        @pl.when(takes_rim)
        def _():
            for copy in rim_copies:
                copy.wait_recv()
            xf[0:8, :] = xrim[...].astype(F32)[RIM - 8 :, :]
            bcf[0:8, :] = bcrim[...].astype(F32)[RIM - 8 :, :]

        @pl.when(jnp.logical_not(takes_rim))
        def _():
            xf[0:8, :] = jnp.zeros((8, inner), F32)
            bcf[0:8, :] = jnp.zeros((8, 2 * STATE), F32)

    with jax.named_scope("f_state"):
        b_conv = conv(bcf, tok, cbc_v, cbcb_v, slice(0, STATE))
        c_conv = conv(bcf, tok, cbc_v, cbcb_v, slice(STATE, 2 * STATE))
        cmat[...] = c_conv
        bmat_t[...] = jnp.transpose(b_conv.astype(F32)).astype(BF16)
        first = conv(xf, RIM, cx_v, cxb_v, slice(0, inner))
        xc[0:RIM, :] = first
        xw[0:RIM, :] = (first.astype(F32) * wrim[...]).astype(BF16)
        plane_copies = []
        for part in range(2):
            lanes = slice(part * half, part * half + half)
            state = dot(bmat_t[...], xw[:, lanes])
            stbuf[part] = state.reshape(plane, rows, half).astype(BF16)
            for d in range(1, plane):
                other = lax.rem(k + d, plane)
                device = peer_in_plane(other)
                copies = [
                    remote(
                        stbuf.at[part, other], p1buf.at[part, k],
                        p1s.at[part, d - 1], p1r.at[part, d - 1], device,
                    )
                ]
                if part == 0:
                    copies.append(
                        remote(dself, dbuf.at[k], d1s.at[d - 1], d1r.at[d - 1], device)
                    )
                for copy in copies:
                    copy.start()
                plane_copies += copies
            p1buf[part, pl.ds(k, 1)] = stbuf[part, pl.ds(k, 1)]
        dbuf[pl.ds(k, 1)] = dself[...][None]

    def inner_tile(tile, carry):
        lanes = pl.ds(pl.multiple_of(tile * 128, 128), 128)
        x_tile = xc[:, lanes]
        parts = []
        for side in range(2):
            head = tile * 2 + side
            row = lax.broadcasted_iota(jnp.int32, (384, tok), 0)
            pick = jnp.where(lax.rem(row, 128) == head, 1.0, 0.0).astype(BF16)
            column = dot(cum3[...], pick)
            gap = jnp.minimum(column - cum_row[pl.ds(head, 1), :], 0.0)
            mixing = (scores[...] * jnp.exp(gap) * step_row[pl.ds(head, 1), :]).astype(BF16)
            parts.append(dot(mixing, x_tile))
        lane = lax.broadcasted_iota(jnp.int32, (tok, 128), 1)
        yg[:, lanes] = jnp.where(lane < HEADDIM, parts[0], parts[1]) * gz[:, lanes]
        return carry

    with jax.named_scope("g_inner"):
        loads[9].wait()
        loads[10].wait()

        def gate_tile(tile, carry):
            lanes = pl.ds(pl.multiple_of(tile * 128, 128), 128)
            gate = silu(z_v[:, lanes].astype(F32))
            gz[:, lanes] = gate
            eg[:, lanes] = gate * dot(ecum2[...], spread(tile, 2))
            return carry

        lax.fori_loop(0, tiles, gate_tile, 0, unroll=2)
        scores[...] = jnp.where(causal, dot(c_conv, b_conv, ((1,), (1,))), 0.0)
        split = EARLY_TILES
        lax.fori_loop(0, split, inner_tile, 0)

    with jax.named_scope("h_plane_wait"):
        for copy in plane_copies:
            copy.wait()

    with jax.named_scope("i_plane_scan"):
        spread_row = lax.broadcasted_iota(jnp.int32, (128, inner), 0)
        spread_col = lax.broadcasted_iota(jnp.int32, (128, inner), 1)
        spread_all = jnp.where(spread_row == lax.div(spread_col, HEADDIM), 1.0, 0.0).astype(F32)
        each = jnp.concatenate([dbuf[i, 0:1, :] for i in range(plane)], axis=0)
        before = [jnp.zeros((1, 128), F32)]
        for i in range(1, plane):
            before.append(before[-1] + each[i - 1 : i, :])
        whole = before[-1] + each[plane - 1 : plane, :]
        before = jnp.concatenate(before, axis=0)
        stacked = jnp.concatenate([each, before], axis=0)
        wide = dot(stacked, spread_all, precision=lax.Precision.HIGHEST)
        factor = jnp.exp(wide[0:plane, :])
        cumd[...] = jnp.exp(wide[plane : 2 * plane, :])
        dplane[...] = jnp.broadcast_to(whole, (8, 128))
        for part in range(2):
            lanes = slice(part * half, part * half + half)
            running = jnp.zeros((rows, half), F32)
            for i in range(plane):
                pbuf[i, :, lanes] = running
                running = factor[i : i + 1, lanes] * running + p1buf[part, i].astype(F32)
            tbuf[:, lanes] = running.astype(BF16)
            qst[:, lanes] = running

    def group_copies(slot, d):
        device = peer_along(z + d)
        return (
            remote(tbuf, abuf.at[slot], as_.at[d - 1], ar.at[slot], device),
            remote(dplane, adec.at[slot], ds_.at[d - 1], dr.at[slot], device),
        )

    group_sends = [(i, d) for i in range(last_size - 1) for d in range(last_size - 1 - i, 0, -1)]

    def sends_group(slot, d):
        return jnp.logical_and(zl == slot, zl + d < size)

    with jax.named_scope("j_group_send"):
        for d in range(1, last_size + 1):

            @pl.when(d <= reach)
            def _():
                pl.semaphore_wait(ready.at[d - 1], 1)

        for slot, d in group_sends:

            @pl.when(sends_group(slot, d))
            def _():
                for copy in group_copies(slot, d):
                    copy.start()

    with jax.named_scope("l_group_wait"):

        @pl.when(zl == 0)
        def _():
            pst[...] = jnp.zeros_like(pst)
            fpre[...] = jnp.ones_like(fpre)

        def widened(row):
            return jnp.exp(dot(row, spread_all, precision=lax.Precision.HIGHEST))

        for place in range(1, last_size):

            @pl.when(zl == place)
            def _():
                for slot in range(place):
                    for copy in group_copies(slot, 1):
                        copy.wait_recv()
                prefix = abuf[0].astype(F32)
                decay = adec[0]
                for slot in range(1, place):
                    prefix = widened(adec[slot])[0:1, :] * prefix + abuf[slot].astype(F32)
                    decay = decay + adec[slot]
                pst[...] = prefix
                fpre[...] = widened(decay)
                if place == GROUP - 1:
                    qst[...] = widened(dplane[...])[0:1, :] * prefix + qst[...]
                    fall[...] = widened(decay + dplane[...])

    def chain_copy(d):
        return remote(ebuf, ech, es.at[d - 1], er.at[0], peer_along(z + d))

    def sends_chain(d):
        return jnp.logical_and(hands_on, d <= next_size)

    with jax.named_scope("m_chain"):

        @pl.when(z < GROUP)
        def _():
            ech[...] = jnp.zeros_like(ech)

        @pl.when(z >= GROUP)
        def _():
            chain_copy(1).wait_recv()

        @pl.when(sends_chain(1))
        def _():
            ebuf[...] = (fall[0:1, :] * ech[...].astype(F32) + qst[...]).astype(BF16)

        for d in range(last_size, 0, -1):

            @pl.when(sends_chain(d))
            def _():
                chain_copy(d).start()

    with jax.named_scope("n_back_send"):
        entering = fpre[0:1, :] * ech[...].astype(F32) + pst[...]
        own_rows = pl.ds(pl.multiple_of(k * rows, rows), rows)
        for i in range(plane):
            obuf[i] = (cumd[i : i + 1, :] * entering + pbuf[i]).astype(BF16)
        back = []
        for d in range(1, plane):
            other = lax.rem(k + d, plane)
            back.append(
                remote(
                    obuf.at[other], ent.at[own_rows, :], p3s.at[d - 1], p3r.at[d - 1],
                    peer_in_plane(other),
                )
            )
        for copy in back:
            copy.start()
        ent[own_rows, :] = obuf[pl.ds(k, 1)].reshape(rows, inner)

    with jax.named_scope("n_inner"):
        lax.fori_loop(split, tiles, inner_tile, 0)

    with jax.named_scope("o_back_wait"):

        @pl.when(gives_rim)
        def _():
            for copy in rim_copies:
                copy.wait_send()

        for slot, d in group_sends:

            @pl.when(sends_group(slot, d))
            def _():
                for copy in group_copies(slot, d):
                    copy.wait_send()

        for copy in back:
            copy.wait()

    with jax.named_scope("p_outer"):
        squares = jnp.zeros((tok, 128), F32)
        for tile in range(tiles):
            lanes = slice(tile * 128, tile * 128 + 128)
            gated = yg[:, lanes] + eg[:, lanes] * dot(cmat[...], ent[:, lanes])
            yg[:, lanes] = gated
            squares = squares + gated * gated

    with jax.named_scope("q_norm"):
        nself[...] = dot(
            jnp.ones((8, 128), F32), squares, ((1,), (1,)), precision=lax.Precision.HIGHEST
        )
        shared = [
            remote(
                nself, nbuf.at[d - 1], ns_.at[d - 1], nr_.at[d - 1], peer_head(lax.rem(y + d, ny))
            )
            for d in range(1, ny)
        ]
        for copy in shared:
            copy.start()
        for d in range(last_size, 0, -1):

            @pl.when(sends_chain(d))
            def _():
                chain_copy(d).wait_send()

        for copy in shared:
            copy.wait()
        summed = nself[...]
        for d in range(1, ny):
            summed = summed + nbuf[d - 1]
        inv = lax.rsqrt(summed / (ny * inner) + 1e-05)
        inv = jnp.transpose(jnp.concatenate([inv] * 16, axis=0))

    with jax.named_scope("r_out"):
        for tile in range(tiles):
            lanes = slice(tile * 128, tile * 128 + 128)
            out_ref[:, lanes] = (yg[:, lanes] * inv * nw_v[:, lanes]).astype(BF16)


def local(
    shape,
    x_in,
    bc_in,
    z_in,
    dt_raw,
    dt_bias,
    a_log,
    conv_x,
    conv_bc,
    conv_x_bias,
    conv_bc_bias,
    norm_weight,
):
    nz, nx, nc, ny = shape
    tok, inner = x_in.shape
    heads = dt_raw.shape[0]
    plane = nx * nc
    rows = STATE // plane
    half = inner // 2
    sizes = (nz, nx, nc, ny, tok, heads, inner)
    operands = (
        x_in, bc_in, z_in, dt_raw, dt_bias, a_log, conv_x, conv_bc, conv_x_bias, conv_bc_bias,
        norm_weight,
    )
    v = pltpu.VMEM
    dma = pltpu.SemaphoreType.DMA
    scratch = [v(o.shape if o.ndim > 1 else (1, *o.shape), o.dtype) for o in operands]
    others = max(ny - 1, 1)
    last = nz - GROUP * (nz // GROUP - 1)
    scratch += [
        v((RIM, inner), BF16), v((RIM, 2 * STATE), BF16),
        v((tok + 8, inner), F32), v((tok + 8, 2 * STATE), F32),
        v((tok, inner), BF16), v((tok, inner), BF16), v((RIM, inner), F32),
        v((STATE, tok), BF16), v((tok, STATE), BF16), v((tok, tok), F32),
        v((128, tok), F32), v((16, 128), F32),
        v((128, tok), F32), v((128, tok), F32), v((tok, 256), BF16), v((tok, 256), BF16),
        v((tok, 384), BF16), v((tok, inner), F32), v((tok, inner), F32), v((tok, inner), F32),
        v((2, plane, rows, half), BF16), v((2, plane, rows, half), BF16), v((8, 128), F32),
        v((plane, 8, 128), F32), v((plane, rows, inner), F32), v((plane, inner), F32),
        v((rows, inner), BF16), v((8, 128), F32), v((last - 1, rows, inner), BF16),
        v((last - 1, 8, 128), F32),
        v((rows, inner), F32), v((8, inner), F32), v((rows, inner), F32), v((8, inner), F32),
        v((rows, inner), BF16), v((rows, inner), BF16),
        v((plane, rows, inner), BF16), v((STATE, inner), BF16),
        v((8, tok), F32), v((others, 8, tok), F32),
        dma((11,)), dma((2,)), dma((2,)),
        dma((2, plane - 1)), dma((2, plane - 1)), dma((plane - 1,)), dma((plane - 1,)),
        dma((last - 1,)), dma((last - 1,)), dma((last - 1,)), dma((last - 1,)),
        dma((last,)), dma((1,)),
        dma((plane - 1,)), dma((plane - 1,)), dma((others,)), dma((others,)),
        pltpu.SemaphoreType.REGULAR((last,)),
    ]
    return pl.pallas_call(
        functools.partial(layer_kernel, sizes),
        out_shape=pltpu.VMEM((tok, inner), BF16),
        in_specs=[pl.BlockSpec(memory_space=pltpu.HBM)] * 11,
        out_specs=pl.BlockSpec(memory_space=pltpu.VMEM),
        scratch_shapes=scratch,
        compiler_params=pltpu.CompilerParams(
            collective_id=0, has_side_effects=True, vmem_limit_bytes=66000000
        ),
        name="layer",
    )(*operands)


def build(mesh, shape):
    torus = Mesh(mesh.devices.reshape(shape), AXES)
    return jax.shard_map(
        functools.partial(local, shape),
        mesh=torus,
        in_specs=(
            P(SEQ, "head"),
            P(SEQ, None),
            P(SEQ, "head"),
            P("head", SEQ),
            P("head"),
            P("head"),
            P(None, "head"),
            P(),
            P("head"),
            P(),
            P("head"),
        ),
        out_specs=P(SEQ, "head"),
        check_vma=False,
    )


def solution(mesh):
    return build(mesh, (16, 4, 2, mesh.shape["head"]))
```

```python
import functools

import jax
import jax.numpy as jnp
from jax import lax
from jax.experimental import pallas as pl
from jax.experimental.pallas import tpu as pltpu
from jax.sharding import Mesh
from jax.sharding import PartitionSpec as P

HEADDIM = 64
STATE = 128
CONV = 4
RIM = 16
GROUP = 3
EARLY_TILES = 6
EARLY_CONV = 4
AXES = ("seq_0", "seq_1", "seq_2", "head")
SEQ = AXES[:3]
F32 = jnp.float32
BF16 = jnp.bfloat16


def dot(a, b, contract=((1,), (0,)), precision=None):
    return lax.dot_general(
        a, b, (contract, ((), ())), preferred_element_type=F32, precision=precision
    )


def silu(value):
    half = 0.5 * value
    return half + half * jnp.tanh(half)


def split_two(value):
    high = value.astype(BF16)
    low = (value - high.astype(F32)).astype(BF16)
    return jnp.concatenate([high, low], axis=1)


def split_three(value):
    high = value.astype(BF16)
    rest = value - high.astype(F32)
    mid = rest.astype(BF16)
    low = (rest - mid.astype(F32)).astype(BF16)
    return jnp.concatenate([high, mid, low], axis=1)


def layer_kernel(sizes, *refs):
    nz, nx, nc, ny, tok, heads, inner = sizes
    (
        x_hbm, bc_hbm, z_hbm, dt_hbm, bias_hbm, alog_hbm, cx_hbm, cbc_hbm, cxb_hbm, cbcb_hbm,
        nw_hbm, out_ref,
        x_v, bc_v, z_v, dt_v, bias_v, alog_v, cx_v, cbc_v, cxb_v, cbcb_v, nw_v,
        xrim, bcrim, xf, bcf, xc, xw, wrim, bmat_t, cmat, scores, dtp, smallp,
        cum_row, step_row, win2, ecum2, cum3, yg, eg, gz,
        stbuf, p1buf, dself, dbuf, pbuf, cumd, tbuf, dplane, abuf, adec,
        pst, fpre, qst, fall, ebuf, ech, obuf, ent, nself, nbuf,
        in_sem, rim_s, rim_r, p1s, p1r, d1s, d1r, as_, ar, ds_, dr, es, er, p3s, p3r, ns_, nr_,
        ready,
    ) = refs
    tiles = inner // 128
    half = inner // 2
    plane = nx * nc
    rows = STATE // nx
    z = lax.axis_index("seq_0")
    x = lax.axis_index("seq_1")
    c = lax.axis_index("seq_2")
    y = lax.axis_index("head")
    k = x * nc + c
    owner = c == nc - 1
    groups = nz // GROUP
    last_size = nz - GROUP * (groups - 1)
    group = jnp.minimum(lax.div(z, GROUP), groups - 1)
    zl = z - group * GROUP
    hands_on = jnp.logical_and(zl == GROUP - 1, group < groups - 1)

    def remote(source, target, send, recv, device):
        return pltpu.make_async_remote_copy(
            src_ref=source, dst_ref=target, send_sem=send, recv_sem=recv,
            device_id=device, device_id_type=pl.DeviceIdType.MESH,
        )

    def peer_in_plane(other):
        return (z, lax.div(other, nc), lax.rem(other, nc), y)

    def owner_of(other):
        return (z, other, nc - 1, y)

    def owner_lane(shift):
        return lax.rem(x + shift, nx)

    def peer_along(other):
        return (other, x, c, y)

    def peer_head(other):
        return (z, x, c, other)

    last_in_plane = k == plane - 1
    first_in_plane = k == 0
    following = lax.rem(k + 1, plane)
    next_z = jnp.where(last_in_plane, z + 1, z)
    next_dev = (next_z, lax.div(following, nc), lax.rem(following, nc), y)
    gives_rim = jnp.logical_or(z < nz - 1, k < plane - 1)
    takes_rim = jnp.logical_or(z > 0, k > 0)
    size = jnp.where(group == groups - 1, last_size, GROUP)
    next_size = jnp.where(group == groups - 2, last_size, GROUP)
    reach = jnp.where(hands_on, next_size, size - 1 - zl)

    def has_source(d):
        return jnp.logical_and(zl >= d - 1, z >= d)

    with jax.named_scope("a_start"):
        pairs = (
            (x_hbm, x_v), (bc_hbm, bc_v), (dt_hbm, dt_v), (bias_hbm, bias_v), (alog_hbm, alog_v),
            (cx_hbm, cx_v), (cbc_hbm, cbc_v), (cxb_hbm, cxb_v), (cbcb_hbm, cbcb_v), (z_hbm, z_v),
            (nw_hbm, nw_v),
        )
        loads = [
            pltpu.make_async_copy(a, b if len(a.shape) > 1 else b.at[0], in_sem.at[i])
            for i, (a, b) in enumerate(pairs)
        ]
        for i in (2, 3, 4, 0, 5, 7, 1, 6, 8, 9, 10):
            loads[i].start()

        barrier = pltpu.get_barrier_semaphore()

        def greet(device):
            pl.semaphore_signal(
                barrier, inc=1, device_id=device, device_id_type=pl.DeviceIdType.MESH
            )

        for d in range(1, last_size + 1):

            @pl.when(jnp.logical_and(owner, d <= reach))
            def _():
                greet(peer_along(z + d))

        @pl.when(jnp.logical_and(first_in_plane, z > 0))
        def _():
            greet((z - 1, nx - 1, nc - 1, y))

        @pl.when(owner)
        def _():
            for d in range(1, plane):
                greet(peer_in_plane(lax.rem(k + d, plane)))

        @pl.when(jnp.logical_not(owner))
        def _():
            for shift in range(nx):
                greet(owner_of(owner_lane(shift)))

        for d in range(1, ny):
            greet(peer_head(lax.rem(y + d, ny)))
        dtp[...] = jnp.zeros_like(dtp)
        smallp[...] = jnp.zeros_like(smallp)
        xf[0:8, :] = jnp.zeros((8, inner), F32)
        for i in (2, 3, 4):
            loads[i].wait()

    with jax.named_scope("b_dt"):
        dtp[0:heads, :] = dt_v[...]
        smallp[0:1, 0:heads] = bias_v[...]
        smallp[8:9, 0:heads] = alog_v[...]
        raw = jnp.transpose(dtp[...]) + smallp[0:1, :]
        step_t = jnp.maximum(raw, 0.0) + jnp.log1p(jnp.exp(-jnp.abs(raw)))
        decay_t = step_t * (-jnp.exp(smallp[8:9, :]))
        tok_i = lax.broadcasted_iota(jnp.int32, (tok, tok), 0)
        tok_j = lax.broadcasted_iota(jnp.int32, (tok, tok), 1)
        causal = tok_i >= tok_j
        lower = jnp.where(causal, 1.0, 0.0).astype(F32)
        cum_t = dot(lower, decay_t, precision=lax.Precision.HIGHEST)
        cum_row[...] = jnp.transpose(cum_t)
        step_row[...] = jnp.transpose(step_t)
        total = cum_t[tok - 1 : tok, :]
        win2[...] = split_two(jnp.exp(total - cum_t) * step_t)
        ecum2[...] = split_two(jnp.exp(cum_t))
        cum3[...] = split_three(cum_t)
        dself[...] = jnp.broadcast_to(total, dself.shape)

    def spread(tile, depth):
        row = lax.broadcasted_iota(jnp.int32, (128 * depth, 128), 0)
        col = lax.broadcasted_iota(jnp.int32, (128 * depth, 128), 1)
        head = tile * 2 + lax.div(col, HEADDIM)
        return jnp.where(lax.rem(row, 128) == head, 1.0, 0.0).astype(BF16)

    def conv(source, count, taps, bias, lanes):
        running = bias[:, lanes] + taps[0:1, lanes] * source[5 : 5 + count, lanes]
        for offset in range(1, CONV):
            start = 5 + offset
            running = running + taps[offset : offset + 1, lanes] * source[start : start + count, lanes]
        return silu(running).astype(BF16)

    with jax.named_scope("c_conv"):
        for i in (0, 5, 7):
            loads[i].wait()

        def conv_tile(tile, carry):
            lanes = pl.ds(pl.multiple_of(tile * 128, 128), 128)
            xf[8 : 8 + tok, lanes] = x_v[:, lanes].astype(F32)
            x_tile = conv(xf, tok, cx_v, cxb_v, lanes)
            xc[:, lanes] = x_tile
            weight = dot(win2[...], spread(tile, 2))
            wrim[:, lanes] = weight[0:RIM, :]
            xw[:, lanes] = (x_tile.astype(F32) * weight).astype(BF16)
            return carry

        lax.fori_loop(0, EARLY_CONV, conv_tile, 0, unroll=2)
        loads[1].wait()

    with jax.named_scope("d_barrier"):
        extra = jnp.where(jnp.logical_and(last_in_plane, z < nz - 1), 1, 0)
        near = jnp.where(owner, plane - 1 + jnp.minimum(zl + 1, z), nx)
        pl.semaphore_wait(barrier, near + (ny - 1) + extra)

    with jax.named_scope("e_rim"):
        rim_copies = [
            remote(x_v.at[pl.ds(tok - RIM, RIM), :], xrim, rim_s.at[0], rim_r.at[0], next_dev),
            remote(bc_v.at[pl.ds(tok - RIM, RIM), :], bcrim, rim_s.at[1], rim_r.at[1], next_dev),
        ]

        @pl.when(gives_rim)
        def _():
            for copy in rim_copies:
                copy.start()

        for d in range(1, last_size + 1):

            @pl.when(jnp.logical_and(owner, has_source(d)))
            def _():
                pl.semaphore_signal(
                    ready.at[d - 1], inc=1, device_id=peer_along(z - d),
                    device_id_type=pl.DeviceIdType.MESH,
                )

        lax.fori_loop(EARLY_CONV, tiles, conv_tile, 0, unroll=2)
        for i in (6, 8):
            loads[i].wait()
        bcf[8 : 8 + tok, :] = bc_v[...].astype(F32)

        @pl.when(takes_rim)
        def _():
            for copy in rim_copies:
                copy.wait_recv()
            xf[0:8, :] = xrim[...].astype(F32)[RIM - 8 :, :]
            bcf[0:8, :] = bcrim[...].astype(F32)[RIM - 8 :, :]

        @pl.when(jnp.logical_not(takes_rim))
        def _():
            xf[0:8, :] = jnp.zeros((8, inner), F32)
            bcf[0:8, :] = jnp.zeros((8, 2 * STATE), F32)

    with jax.named_scope("f_state"):
        b_conv = conv(bcf, tok, cbc_v, cbcb_v, slice(0, STATE))
        c_conv = conv(bcf, tok, cbc_v, cbcb_v, slice(STATE, 2 * STATE))
        cmat[...] = c_conv
        bmat_t[...] = jnp.transpose(b_conv.astype(F32)).astype(BF16)
        first = conv(xf, RIM, cx_v, cxb_v, slice(0, inner))
        xc[0:RIM, :] = first
        xw[0:RIM, :] = (first.astype(F32) * wrim[...]).astype(BF16)

        def to_owner(part, shift):
            lane = owner_lane(shift)
            return remote(
                stbuf.at[part, lane], p1buf.at[part, k], p1s.at[part, shift], p1r.at[part, k],
                owner_of(lane),
            )

        def decay_to_owner(shift):
            return remote(dself, dbuf.at[k], d1s.at[shift], d1r.at[k], owner_of(owner_lane(shift)))

        for part in range(2):
            lanes = slice(part * half, part * half + half)
            state = dot(bmat_t[...], xw[:, lanes])
            stbuf[part] = state.reshape(nx, rows, half).astype(BF16)
            for shift in range(1, nx):
                if part == 0:
                    decay_to_owner(shift).start()
                to_owner(part, shift).start()

            @pl.when(jnp.logical_not(owner))
            def _():
                if part == 0:
                    decay_to_owner(0).start()
                to_owner(part, 0).start()

            @pl.when(owner)
            def _():
                p1buf[part, pl.ds(k, 1)] = stbuf[part, pl.ds(x, 1)]

        @pl.when(owner)
        def _():
            dbuf[pl.ds(k, 1)] = dself[...][None]

    def inner_tile(tile, carry):
        lanes = pl.ds(pl.multiple_of(tile * 128, 128), 128)
        x_tile = xc[:, lanes]
        parts = []
        for side in range(2):
            head = tile * 2 + side
            row = lax.broadcasted_iota(jnp.int32, (384, tok), 0)
            pick = jnp.where(lax.rem(row, 128) == head, 1.0, 0.0).astype(BF16)
            column = dot(cum3[...], pick)
            gap = jnp.minimum(column - cum_row[pl.ds(head, 1), :], 0.0)
            mixing = (scores[...] * jnp.exp(gap) * step_row[pl.ds(head, 1), :]).astype(BF16)
            parts.append(dot(mixing, x_tile))
        lane = lax.broadcasted_iota(jnp.int32, (tok, 128), 1)
        yg[:, lanes] = jnp.where(lane < HEADDIM, parts[0], parts[1]) * gz[:, lanes]
        return carry

    with jax.named_scope("g_inner"):
        loads[9].wait()
        loads[10].wait()

        def gate_tile(tile, carry):
            lanes = pl.ds(pl.multiple_of(tile * 128, 128), 128)
            gate = silu(z_v[:, lanes].astype(F32))
            gz[:, lanes] = gate
            eg[:, lanes] = gate * dot(ecum2[...], spread(tile, 2))
            return carry

        lax.fori_loop(0, tiles, gate_tile, 0, unroll=2)
        scores[...] = jnp.where(causal, dot(c_conv, b_conv, ((1,), (1,))), 0.0)
        split = EARLY_TILES
        lax.fori_loop(0, split, inner_tile, 0)

    spread_row = lax.broadcasted_iota(jnp.int32, (128, inner), 0)
    spread_col = lax.broadcasted_iota(jnp.int32, (128, inner), 1)
    spread_all = jnp.where(spread_row == lax.div(spread_col, HEADDIM), 1.0, 0.0).astype(F32)

    def widened(row):
        return jnp.exp(dot(row, spread_all, precision=lax.Precision.HIGHEST))

    def group_copies(slot, d):
        device = peer_along(z + d)
        return (
            remote(tbuf, abuf.at[slot], as_.at[d - 1], ar.at[slot], device),
            remote(dplane, adec.at[slot], ds_.at[d - 1], dr.at[slot], device),
        )

    group_sends = [(i, d) for i in range(last_size - 1) for d in range(last_size - 1 - i, 0, -1)]

    def sends_group(slot, d):
        return jnp.logical_and(zl == slot, zl + d < size)

    def chain_copy(part, d):
        return remote(
            ebuf.at[part], ech.at[part], es.at[part, d - 1], er.at[part], peer_along(z + d)
        )

    def sends_chain(d):
        return jnp.logical_and(hands_on, d <= next_size)

    own_rows = pl.ds(pl.multiple_of(x * rows, rows), rows)

    def back_copy(part, d):
        other = lax.rem(k + d, plane)
        return remote(
            obuf.at[part, other], ent.at[part, own_rows, :], p3s.at[part, d - 1], p3r.at[part, x],
            peer_in_plane(other),
        )

    def back_from(part, shift):
        lane = owner_lane(shift)
        return remote(
            obuf.at[part, 0], ent.at[part, own_rows, :], p3s.at[part, 0], p3r.at[part, lane],
            owner_of(lane),
        )

    @pl.when(owner)
    def _():
        with jax.named_scope("h_plane_wait"):
            for d in range(1, plane):
                source = lax.rem(k + d, plane)
                remote(
                    dself, dbuf.at[source], d1s.at[0], d1r.at[source], peer_in_plane(source)
                ).wait_recv()
                for part in range(2):
                    remote(
                        stbuf.at[part, 0], p1buf.at[part, source], p1s.at[part, 0],
                        p1r.at[part, source], peer_in_plane(source),
                    ).wait_recv()

        with jax.named_scope("i_plane_scan"):
            each = jnp.concatenate([dbuf[i, 0:1, :] for i in range(plane)], axis=0)
            before = [jnp.zeros((1, 128), F32)]
            for i in range(1, plane):
                before.append(before[-1] + each[i - 1 : i, :])
            whole = before[-1] + each[plane - 1 : plane, :]
            before = jnp.concatenate(before, axis=0)
            wide = widened(jnp.concatenate([each, before], axis=0))
            factor = wide[0:plane, :]
            cumd[...] = wide[plane : 2 * plane, :]
            dplane[...] = jnp.broadcast_to(whole, (8, 128))
            for part in range(2):
                lanes = slice(part * half, part * half + half)
                running = jnp.zeros((rows, half), F32)
                for i in range(plane):
                    pbuf[i, :, lanes] = running
                    running = factor[i : i + 1, lanes] * running + p1buf[part, i].astype(F32)
                tbuf[:, lanes] = running.astype(BF16)
                qst[:, lanes] = running

        with jax.named_scope("j_group_send"):
            for d in range(1, last_size + 1):

                @pl.when(d <= reach)
                def _():
                    pl.semaphore_wait(ready.at[d - 1], 1)

            for slot, d in group_sends:

                @pl.when(sends_group(slot, d))
                def _():
                    for copy in group_copies(slot, d):
                        copy.start()

        with jax.named_scope("l_group_wait"):

            @pl.when(zl == 0)
            def _():
                pst[...] = jnp.zeros_like(pst)
                fpre[...] = jnp.ones_like(fpre)

            for place in range(1, last_size):

                @pl.when(zl == place)
                def _():
                    for slot in range(place):
                        for copy in group_copies(slot, 1):
                            copy.wait_recv()
                    prefix = abuf[0].astype(F32)
                    decay = adec[0]
                    for slot in range(1, place):
                        prefix = widened(adec[slot])[0:1, :] * prefix + abuf[slot].astype(F32)
                        decay = decay + adec[slot]
                    pst[...] = prefix
                    fpre[...] = widened(decay)
                    if place == GROUP - 1:
                        qst[...] = widened(dplane[...])[0:1, :] * prefix + qst[...]
                        fall[...] = widened(decay + dplane[...])

        for part in range(2):
            lanes = slice(part * half, part * half + half)
            with jax.named_scope("m_chain"):

                @pl.when(group == 0)
                def _():
                    ech[part] = jnp.zeros((rows, half), BF16)

                @pl.when(group > 0)
                def _():
                    chain_copy(part, 1).wait_recv()

                @pl.when(hands_on)
                def _():
                    ebuf[part] = (
                        fall[0:1, lanes] * ech[part].astype(F32) + qst[:, lanes]
                    ).astype(BF16)
                    chain_copy(part, GROUP).start()

        with jax.named_scope("m_hand_on"):
            for d in range(last_size, 0, -1):
                if d != GROUP:

                    @pl.when(sends_chain(d))
                    def _():
                        for part in range(2):
                            chain_copy(part, d).start()

        with jax.named_scope("n_back_send"):
            for part in range(2):
                lanes = slice(part * half, part * half + half)
                entering = fpre[0:1, lanes] * ech[part].astype(F32) + pst[:, lanes]
                for i in range(plane):
                    obuf[part, i] = (
                        cumd[i : i + 1, lanes] * entering + pbuf[i, :, lanes]
                    ).astype(BF16)
                for d in range(1, plane):
                    back_copy(part, d).start()
                ent[part, own_rows, :] = obuf[part, pl.ds(k, 1)].reshape(rows, half)

    with jax.named_scope("n_inner"):
        lax.fori_loop(split, tiles, inner_tile, 0)

    with jax.named_scope("o_back_wait"):

        @pl.when(gives_rim)
        def _():
            for copy in rim_copies:
                copy.wait_send()

        for shift in range(1, nx):
            decay_to_owner(shift).wait_send()
            for part in range(2):
                to_owner(part, shift).wait_send()

        @pl.when(jnp.logical_not(owner))
        def _():
            decay_to_owner(0).wait_send()
            for part in range(2):
                to_owner(part, 0).wait_send()

        @pl.when(owner)
        def _():
            for slot, d in group_sends:

                @pl.when(sends_group(slot, d))
                def _():
                    for copy in group_copies(slot, d):
                        copy.wait_send()

            for part in range(2):
                for d in range(1, plane):
                    back_copy(part, d).wait_send()

        for part in range(2):

            @pl.when(jnp.logical_not(owner))
            def _():
                back_from(part, 0).wait_recv()

            for shift in range(1, nx):
                back_from(part, shift).wait_recv()

    with jax.named_scope("p_outer"):
        squares = jnp.zeros((tok, 128), F32)
        for tile in range(tiles):
            lanes = slice(tile * 128, tile * 128 + 128)
            part, begin = divmod(tile * 128, half)
            outer = dot(cmat[...], ent[part, :, begin : begin + 128])
            gated = yg[:, lanes] + eg[:, lanes] * outer
            yg[:, lanes] = gated
            squares = squares + gated * gated

    with jax.named_scope("q_norm"):
        nself[...] = dot(
            jnp.ones((8, 128), F32), squares, ((1,), (1,)), precision=lax.Precision.HIGHEST
        )
        shared = [
            remote(
                nself, nbuf.at[d - 1], ns_.at[d - 1], nr_.at[d - 1], peer_head(lax.rem(y + d, ny))
            )
            for d in range(1, ny)
        ]
        for copy in shared:
            copy.start()
        @pl.when(owner)
        def _():
            for d in range(last_size, 0, -1):

                @pl.when(sends_chain(d))
                def _():
                    for part in range(2):
                        chain_copy(part, d).wait_send()

        for copy in shared:
            copy.wait()
        summed = nself[...]
        for d in range(1, ny):
            summed = summed + nbuf[d - 1]
        inv = lax.rsqrt(summed / (ny * inner) + 1e-05)
        inv = jnp.transpose(jnp.concatenate([inv] * 16, axis=0))

    with jax.named_scope("r_out"):
        for tile in range(tiles):
            lanes = slice(tile * 128, tile * 128 + 128)
            out_ref[:, lanes] = (yg[:, lanes] * inv * nw_v[:, lanes]).astype(BF16)


def local(
    shape,
    x_in,
    bc_in,
    z_in,
    dt_raw,
    dt_bias,
    a_log,
    conv_x,
    conv_bc,
    conv_x_bias,
    conv_bc_bias,
    norm_weight,
):
    nz, nx, nc, ny = shape
    tok, inner = x_in.shape
    heads = dt_raw.shape[0]
    plane = nx * nc
    rows = STATE // nx
    half = inner // 2
    sizes = (nz, nx, nc, ny, tok, heads, inner)
    operands = (
        x_in, bc_in, z_in, dt_raw, dt_bias, a_log, conv_x, conv_bc, conv_x_bias, conv_bc_bias,
        norm_weight,
    )
    v = pltpu.VMEM
    dma = pltpu.SemaphoreType.DMA
    scratch = [v(o.shape if o.ndim > 1 else (1, *o.shape), o.dtype) for o in operands]
    others = max(ny - 1, 1)
    last = nz - GROUP * (nz // GROUP - 1)
    scratch += [
        v((RIM, inner), BF16), v((RIM, 2 * STATE), BF16),
        v((tok + 8, inner), F32), v((tok + 8, 2 * STATE), F32),
        v((tok, inner), BF16), v((tok, inner), BF16), v((RIM, inner), F32),
        v((STATE, tok), BF16), v((tok, STATE), BF16), v((tok, tok), F32),
        v((128, tok), F32), v((16, 128), F32),
        v((128, tok), F32), v((128, tok), F32), v((tok, 256), BF16), v((tok, 256), BF16),
        v((tok, 384), BF16), v((tok, inner), F32), v((tok, inner), F32), v((tok, inner), F32),
        v((2, nx, rows, half), BF16), v((2, plane, rows, half), BF16), v((8, 128), F32),
        v((plane, 8, 128), F32), v((plane, rows, inner), F32), v((plane, inner), F32),
        v((rows, inner), BF16), v((8, 128), F32), v((last - 1, rows, inner), BF16),
        v((last - 1, 8, 128), F32),
        v((rows, inner), F32), v((8, inner), F32), v((rows, inner), F32), v((8, inner), F32),
        v((2, rows, half), BF16), v((2, rows, half), BF16),
        v((2, plane, rows, half), BF16), v((2, STATE, half), BF16),
        v((8, tok), F32), v((others, 8, tok), F32),
        dma((11,)), dma((2,)), dma((2,)),
        dma((2, nx)), dma((2, plane)), dma((nx,)), dma((plane,)),
        dma((last - 1,)), dma((last - 1,)), dma((last - 1,)), dma((last - 1,)),
        dma((2, last)), dma((2,)),
        dma((2, plane - 1)), dma((2, nx)), dma((others,)), dma((others,)),
        pltpu.SemaphoreType.REGULAR((last,)),
    ]
    return pl.pallas_call(
        functools.partial(layer_kernel, sizes),
        out_shape=pltpu.VMEM((tok, inner), BF16),
        in_specs=[pl.BlockSpec(memory_space=pltpu.HBM)] * 11,
        out_specs=pl.BlockSpec(memory_space=pltpu.VMEM),
        scratch_shapes=scratch,
        compiler_params=pltpu.CompilerParams(
            collective_id=0, has_side_effects=True, vmem_limit_bytes=66000000
        ),
        name="layer",
    )(*operands)


def build(mesh, shape):
    torus = Mesh(mesh.devices.reshape(shape), AXES)
    return jax.shard_map(
        functools.partial(local, shape),
        mesh=torus,
        in_specs=(
            P(SEQ, "head"),
            P(SEQ, None),
            P(SEQ, "head"),
            P("head", SEQ),
            P("head"),
            P("head"),
            P(None, "head"),
            P(),
            P("head"),
            P(),
            P("head"),
        ),
        out_specs=P(SEQ, "head"),
        check_vma=False,
    )


def solution(mesh):
    return build(mesh, (16, 4, 2, mesh.shape["head"]))
```
